32 devices in a mesh: dp: 8 (over y, x, core), mp: 4 (over z).
Axes of the slice: x: 2, y: 2, z: 4, core: 2. Of those that a mesh axis runs over, the one named last changes fastest.
Arguments:
- tokens: bfloat16 [1024, 8192], P(('dp', 'mp')), parts along dimension 0, may hold values from -6 to 6
- norm_gain: float32 [8192], replicated, may hold values from 0.5 to 1.5
- qkv_weight: bfloat16 [8192, 10240], P(None, 'mp'), may hold values from -0.0625 to 0.0625
- qkv_bias: float32 [10240], P('mp'), may hold values from -3 to 3
- qkv_grad: bfloat16 [1024, 10240], P('dp', 'mp'), parts along dimension 0, may hold values from -6 to 6
Outputs:
- qkv: bfloat16 [1024, 10240], P('dp', 'mp'), parts along dimension 0
- tokens_grad: float32 [1024, 8192], P(('dp', 'mp')), parts along dimension 0
- gain_grad: float32 [65536], P('dp'), parts along dimension 0
- bias_grad: float32 [81920], P(('dp', 'mp')), parts along dimension 0
The draws below stay inside these ranges and needn't reach their ends.
There are 8 independent parts, one for each index of `dp`. The reference program is written for one: setup_inputs(seed, part) draws one part's arguments, and reference() takes and returns one part's arrays. A program takes and returns all parts, laid end to end along the dimension named above; an argument that names none is the same for every part. Nothing has to cross between parts.
All inputs are finite; a program needn't handle non-finite values.
Results may differ from the reference program's by a relative error of at most 0.0046.
Values may be sent and summed in bfloat16 or wider, within the bound.
A program may use at most 128 MiB of HBM per device.

```python
import jax
import jax.numpy as jnp
from jax import lax

D = 8192
HEAD_DIM = 128
GROUP = 10
COLS = 10240
STRIDE = 8192
TOK_DEV = 32
TOKENS = 128


def strengthened(values, own_key, source, target, shards_of, factor):
    def block_of(axis_at):
        return (jnp.arange(values.shape[axis_at]) // (values.shape[axis_at] // shards_of)).reshape((-1,) + (1,) * (values.ndim - 1 - axis_at))

    first = jax.random.permutation(own_key, shards_of)[block_of(target)]
    far = (block_of(target) + shards_of // 2) % shards_of
    return jnp.where((block_of(source) == first) | (block_of(source) == far), factor * values, values)


def shard_levels(stream_key, shape, cuts, smallest, top_value):
    def one(axis_at, blocks):
        heights = jax.random.uniform(jax.random.fold_in(jax.random.fold_in(stream_key, 6), axis_at), (blocks,), jnp.float32, smallest / len(cuts), top_value / len(cuts))
        return jnp.repeat(jnp.exp(heights), shape[axis_at] // blocks).reshape((-1,) + (1,) * (len(shape) - axis_at - 1))

    factor_of = one(*cuts[0])
    for cut in cuts[1:]:
        factor_of = factor_of * one(*cut)
    return factor_of


def gaussian(own_key, dims, deviation, bound, shards=(), kind=jnp.bfloat16):
    array = deviation * jax.random.normal(own_key, dims, jnp.float32)
    if shards:
        array = array * shard_levels(own_key, dims, shards, -0.22, 0.18)
    return jnp.clip(array, -bound, bound).astype(kind)


def gaussian_with(stream_key, extent, deviation, limit, cuts, heavy, kind=jnp.bfloat16):
    array = deviation * jax.random.normal(stream_key, extent, jnp.float32)
    if cuts:
        array = array * shard_levels(stream_key, extent, cuts, -0.22, 0.18)
    return jnp.clip(strengthened(array, jax.random.fold_in(stream_key, 3), *heavy), -limit, limit).astype(kind)


def setup_inputs(seed: int = 0, part: int = 0) -> dict:
    key_list = jax.random.split(jax.random.key(seed), 6)
    part_keys = jax.random.split(jax.random.fold_in(key_list[5], part), 6)
    return {
        "tokens": gaussian(part_keys[0], (TOKENS, D), 1.0, 6.0, ((0, 4),)),
        "norm_gain": jnp.clip(1.0 + 0.1 * jax.random.normal(key_list[1], (D,), jnp.float32), 0.5, 1.5),
        "qkv_weight": gaussian(key_list[2], (D, COLS), D ** -0.5, 0.0625, ((1, 4),)),
        "qkv_bias": gaussian(key_list[3], (COLS,), 0.5, 3.0, ((0, 4),), jnp.float32),
        "qkv_grad": gaussian_with(part_keys[4], (TOKENS, COLS), 1.0, 6.0, ((1, 4),), (1, 0, 4, 2.0)),
    }


def rotate_heads(joined, first_col, position, sign):
    rows, cols = joined.shape
    heads = cols // HEAD_DIM
    half = HEAD_DIM // 2
    parts = joined.reshape(rows, heads, 2, half)
    inverse = jnp.exp(-jnp.log(jnp.float32(1000000.0)) * (2.0 * jnp.arange(half).astype(jnp.float32) / HEAD_DIM))
    angle = position.astype(jnp.float32)[:, None] * inverse[None, :]
    cosine = jnp.cos(angle)[:, None, :]
    sine = sign * jnp.sin(angle)[:, None, :]
    first = parts[:, :, 0, :]
    second = parts[:, :, 1, :]
    turned = jnp.stack([first * cosine - second * sine, second * cosine + first * sine], axis=2)
    head_index = first_col // HEAD_DIM + jnp.arange(heads)
    rotated = head_index % GROUP != GROUP - 1
    result = jnp.where(rotated[None, :, None, None], turned, parts)
    return result.reshape(rows, cols)

def reference(tokens, norm_gain, qkv_weight, qkv_bias, qkv_grad):
    row_index = jnp.arange(TOKENS).astype(jnp.int32)
    position = row_index // TOK_DEV * STRIDE + row_index % TOK_DEV
    values = tokens.astype(jnp.float32)
    scale = lax.rsqrt(lax.optimization_barrier(jnp.mean(values * values, axis=1, keepdims=True)) + 1e-06)
    normed = (values * scale * norm_gain[None, :]).astype(jnp.bfloat16)
    joined = jnp.dot(normed, qkv_weight, preferred_element_type=jnp.float32) + qkv_bias[None, :]
    qkv = rotate_heads(joined, 0, position, 1.0).astype(jnp.bfloat16)
    joined_grad = rotate_heads(qkv_grad.astype(jnp.float32), 0, position, -1.0)
    bias_grad = lax.optimization_barrier(jnp.sum(joined_grad, axis=0))
    joined_low = joined_grad.astype(jnp.bfloat16)
    normed_grad = lax.dot_general(joined_low, qkv_weight, (((1,), (1,)), ((), ())), preferred_element_type=jnp.float32)
    gain_grad = lax.optimization_barrier(jnp.sum(normed_grad * values * scale, axis=0))
    inner = lax.optimization_barrier(jnp.mean(norm_gain[None, :] * normed_grad * values, axis=1, keepdims=True))
    tokens_grad = scale * norm_gain[None, :] * normed_grad - values * scale * scale * scale * inner
    return (qkv, tokens_grad, gain_grad, bias_grad)
```

```python
import functools

import jax
import jax.numpy as jnp
import numpy as np
from jax import lax
from jax.experimental import pallas as pl
from jax.experimental.pallas import tpu as pltpu
from jax.sharding import PartitionSpec as P

HEAD_DIM = 128
SEQ_LEN = 32768
GROUP = 10
CHUNKS = 4
TILE_K = 512
MESH = pl.DeviceIdType.MESH


def rope_tables(rows, tok_dev, stride):
    half = HEAD_DIM // 2
    row = np.arange(rows)
    place = (row // tok_dev * stride + row % tok_dev).astype(np.float32)
    inverse = np.exp(
        -np.log(np.float32(1000000.0))
        * (np.float32(2.0) * np.arange(half).astype(np.float32) / np.float32(HEAD_DIM))
    ).astype(np.float32)
    angle = (place[:, None] * inverse[None, :]).astype(np.float32)
    cosine, sine = np.cos(angle).astype(np.float32), np.sin(angle).astype(np.float32)
    return np.concatenate([cosine, cosine], 1), np.concatenate([-sine, sine], 1)


def kernel(
    n,
    tok_h, gain_h, w_h, bias_h, grad_h, cos_h, sin_h,
    qkv_h, tg_h, gg_ref, bg_ref,
    tok, gain, w, bias, grad, cos, sin,
    low, part, held, run, acc, qkv, ng, tg, scale_ref, gsend, grecv,
    in_sem, w_sem, out_sem, send_sem, recv_sem, gsend_sem, grecv_sem,
):
    me = lax.axis_index("mp")
    rows, depth = tok.shape
    width = w.shape[1]
    heads = width // HEAD_DIM
    span = depth // CHUNKS
    tiles = depth // TILE_K
    per = tiles // CHUNKS
    f32 = jnp.float32

    loads = []
    for i, (src, dst) in enumerate(
        ((tok_h, tok), (gain_h, gain), (grad_h, grad), (cos_h, cos), (sin_h, sin), (bias_h, bias))
    ):
        c = pltpu.make_async_copy(src, dst, in_sem.at[i])
        c.start()
        loads.append(c)

    def w_copy(i):
        k = pl.ds(pl.multiple_of(i * TILE_K, TILE_K), TILE_K)
        return pltpu.make_async_copy(w_h.at[k, :], w.at[k, :], w_sem.at[i])

    @pl.loop(0, tiles)
    def _(i):
        w_copy(i).start()

    barrier = pltpu.get_barrier_semaphore()
    for k in range(1, n):
        pl.semaphore_signal(
            barrier, inc=1, device_id={"mp": lax.rem(me + k, n)}, device_id_type=MESH
        )

    def block(s):
        return pl.ds(pl.multiple_of(s * rows, rows), rows)

    def cols(c):
        return pl.ds(pl.multiple_of(c * span, span), span)

    loads[0].wait()
    loads[1].wait()
    total = jnp.zeros((rows, 1), f32)
    for c in range(CHUNKS):
        v = tok[:, c * span:(c + 1) * span].astype(f32)
        total = total + jnp.sum(v * v, axis=1, keepdims=True)
    scale = lax.rsqrt(total / depth + 1e-06)
    scale_ref[...] = jnp.broadcast_to(scale, scale_ref.shape)
    for c in range(CHUNKS):
        ks = slice(c * span, (c + 1) * span)
        held[block(me), ks] = (tok[:, ks].astype(f32) * scale * gain[:, ks]).astype(jnp.bfloat16)
    pl.semaphore_wait(barrier, n - 1)

    def transfer(way, buf, at, j, c):
        ref = buf.at[block(at), cols(c)]
        return pltpu.make_async_remote_copy(
            src_ref=ref,
            dst_ref=ref,
            send_sem=send_sem.at[way, j, c],
            recv_sem=recv_sem.at[way, j, c],
            device_id={"mp": lax.rem(me + (1 if way == 0 else n - 1), n)},
            device_id_type=MESH,
        )

    has_right, has_left = me < n - 1, me > 0

    def step(j, c):
        for way, goes, comes, back in ((0, has_right, has_left, me), (1, has_left, has_right, n - 1 - me)):
            @pl.when(comes)
            def _():
                transfer(way, held, 0, j - 1, c).wait_recv()

            @pl.when(goes)
            def _():
                @pl.when(j <= back)
                def _():
                    transfer(way, held, me - j if way == 0 else me + j, j, c).start()

                @pl.when(j > back)
                def _():
                    t = n - j + me if way == 0 else j - n + me
                    slot = t + 1 if way == 0 else t

                    @pl.when(comes)
                    def _():
                        value = part[block(t), cols(c)] + run[block(slot), cols(c)].astype(f32)
                        run[block(slot), cols(c)] = value.astype(jnp.bfloat16)

                    @pl.when(jnp.logical_not(comes))
                    def _():
                        run[block(slot), cols(c)] = part[block(t), cols(c)].astype(jnp.bfloat16)

                    transfer(way, run, slot, j, c).start()

    for c in range(CHUNKS):
        for way, goes in ((0, has_right), (1, has_left)):
            @pl.when(goes)
            def _():
                transfer(way, held, me, 0, c).start()

    for l in loads[2:]:
        l.wait()
    for h in range(heads):
        hs = slice(h * HEAD_DIM, (h + 1) * HEAD_DIM)
        x = grad[:, hs].astype(f32)
        turned = x * cos[...] - pltpu.roll(x, HEAD_DIM // 2, 1) * sin[...]
        plain = lax.rem(me * heads + h, GROUP) == GROUP - 1
        x = jnp.where(plain, x, turned)
        bg_ref[:, hs] = jnp.sum(x, axis=0, keepdims=True)
        low[:, hs] = x.astype(jnp.bfloat16)

    def backward(c):
        @pl.loop(0, per)
        def _(i):
            at = c * per + i
            w_copy(at).wait()
            k = pl.ds(pl.multiple_of(at * TILE_K, TILE_K), TILE_K)
            part[:, k] = lax.dot_general(
                low[...], w[k, :], (((1,), (1,)), ((), ())), preferred_element_type=f32
            )

    @pl.loop(0, CHUNKS)
    def _(c):
        backward(c)

        @pl.when(c > 0)
        def _():
            step(1, c - 1)

    step(1, CHUNKS - 1)

    @pl.loop(2, n - 1)
    def _(j):
        @pl.loop(0, CHUNKS)
        def _(c):
            step(j, c)

    tile_n = 640 if width % 640 == 0 else HEAD_DIM
    tiles_n = width // tile_n

    @pl.loop(0, CHUNKS)
    def _(c):
        step(n - 1, c)

        @pl.loop(0, tiles_n)
        def _(i):
            ns = pl.ds(pl.multiple_of(i * tile_n, tile_n), tile_n)
            value = jnp.dot(held[:, cols(c)], w[cols(c), ns], preferred_element_type=f32)

            @pl.when(c == 0)
            def _():
                acc[:, ns] = value

            @pl.when(c > 0)
            def _():
                acc[:, ns] += value

    for h in range(heads):
        hs = slice(h * HEAD_DIM, (h + 1) * HEAD_DIM)
        x = acc[:, hs] + bias[:, hs]
        turned = x * cos[...] + pltpu.roll(x, HEAD_DIM // 2, 1) * sin[...]
        plain = lax.rem(me * heads + h, GROUP) == GROUP - 1
        qkv[:, hs] = jnp.where(plain, x, turned).astype(jnp.bfloat16)
    out_q = pltpu.make_async_copy(qkv, qkv_h, out_sem.at[0])
    out_q.start()

    def gain_copy(k, c):
        return pltpu.make_async_remote_copy(
            src_ref=gsend.at[c],
            dst_ref=grecv.at[k - 1, c],
            send_sem=gsend_sem.at[k - 1, c],
            recv_sem=grecv_sem.at[k - 1, c],
            device_id={"mp": lax.rem(me + k, n)},
            device_id_type=MESH,
        )

    scale = scale_ref[:, :1]
    inner = jnp.zeros((rows, 1), f32)
    piece = span // 8
    for c in range(CHUNKS):
        ks = slice(c * span, (c + 1) * span)
        ng[:, ks] = part[block(me), ks]
        for way, comes, slot in ((0, has_left, me + 1), (1, has_right, me)):
            @pl.when(comes)
            def _():
                transfer(way, run, slot, n - 1, c).wait_recv()
                ng[:, ks] += run[block(slot), ks].astype(f32)

        product = ng[:, ks] * tok[:, ks].astype(f32)
        gg = jnp.sum(product * scale, axis=0, keepdims=True)
        inner = inner + jnp.sum(product * gain[:, ks], axis=1, keepdims=True)
        for i in range(8):
            gsend[c, i:i + 1, :] = gg[:, i * piece:(i + 1) * piece]
        for k in range(1, n):
            gain_copy(k, c).start()

    weight = scale * scale * scale * (inner / depth)
    for c in range(CHUNKS):
        ks = slice(c * span, (c + 1) * span)
        tg[:, ks] = scale * gain[:, ks] * ng[:, ks] - tok[:, ks].astype(f32) * weight
    out_t = pltpu.make_async_copy(tg, tg_h, out_sem.at[1])
    out_t.start()

    for c in range(CHUNKS):
        total = gsend[c]
        for k in range(1, n):
            gain_copy(k, c).wait_recv()
            total = total + grecv[k - 1, c]
        for i in range(8):
            at = c * span + i * piece
            gg_ref[:, at:at + piece] = total[i:i + 1, :]

    @pl.loop(0, n)
    def _(j):
        @pl.loop(0, CHUNKS)
        def _(c):
            for way, goes in ((0, has_right), (1, has_left)):
                @pl.when(goes)
                def _():
                    transfer(way, held, 0, j, c).wait_send()

    for c in range(CHUNKS):
        for k in range(1, n):
            gain_copy(k, c).wait_send()
    out_q.wait()
    out_t.wait()


def shards(n, tokens, norm_gain, qkv_weight, qkv_bias, qkv_grad):
    rows, depth = tokens.shape
    every, width = qkv_grad.shape
    cosine, sine = rope_tables(every, rows, SEQ_LEN // n)
    bf16, f32 = jnp.bfloat16, jnp.float32
    span = depth // CHUNKS
    dma = pltpu.SemaphoreType.DMA
    hbm = pl.BlockSpec(memory_space=pl.ANY)
    vmem = pl.BlockSpec(memory_space=pltpu.VMEM)
    qkv, tokens_grad, gain_grad, bias_grad = pl.pallas_call(
        functools.partial(kernel, n),
        out_shape=(
            jax.ShapeDtypeStruct((every, width), bf16),
            jax.ShapeDtypeStruct((rows, depth), f32),
            jax.ShapeDtypeStruct((1, depth), f32),
            jax.ShapeDtypeStruct((1, width), f32),
        ),
        in_specs=[hbm] * 7,
        out_specs=(hbm, hbm, vmem, vmem),
        scratch_shapes=[
            pltpu.VMEM((rows, depth), bf16),
            pltpu.VMEM((1, depth), f32),
            pltpu.VMEM((depth, width), bf16),
            pltpu.VMEM((1, width), f32),
            pltpu.VMEM((every, width), bf16),
            pltpu.VMEM((every, HEAD_DIM), f32),
            pltpu.VMEM((every, HEAD_DIM), f32),
            pltpu.VMEM((every, width), bf16),
            pltpu.VMEM((every, depth), f32),
            pltpu.VMEM((every, depth), bf16),
            pltpu.VMEM((every + rows, depth), bf16),
            pltpu.VMEM((every, width), f32),
            pltpu.VMEM((every, width), bf16),
            pltpu.VMEM((rows, depth), f32),
            pltpu.VMEM((rows, depth), f32),
            pltpu.VMEM((rows, HEAD_DIM), f32),
            pltpu.VMEM((CHUNKS, 8, span // 8), f32),
            pltpu.VMEM((n - 1, CHUNKS, 8, span // 8), f32),
            dma((6,)),
            dma((depth // TILE_K,)),
            dma((2,)),
            dma((2, n, CHUNKS)),
            dma((2, n, CHUNKS)),
            dma((n - 1, CHUNKS)),
            dma((n - 1, CHUNKS)),
        ],
        compiler_params=pltpu.CompilerParams(
            collective_id=0, has_side_effects=True, vmem_limit_bytes=65000000
        ),
        cost_estimate=pl.CostEstimate(
            flops=4 * every * depth * width, bytes_accessed=2 * depth * width, transcendentals=0
        ),
    )(
        tokens, norm_gain.reshape(1, depth), qkv_weight, qkv_bias.reshape(1, width), qkv_grad,
        jnp.asarray(cosine), jnp.asarray(sine),
    )
    return qkv, tokens_grad, gain_grad.reshape(depth), bias_grad.reshape(width)


def solution(mesh):
    in_specs = (P(("dp", "mp"), None), P(), P(None, "mp"), P("mp"), P("dp", "mp"))
    out_specs = (P("dp", "mp"), P(("dp", "mp"), None), P("dp"), P(("dp", "mp")))
    body = functools.partial(shards, mesh.shape["mp"])
    return jax.shard_map(body, mesh=mesh, in_specs=in_specs, out_specs=out_specs, check_vma=False)
```

```python
import functools

import jax
import jax.numpy as jnp
import numpy as np
from jax import lax
from jax.experimental import pallas as pl
from jax.experimental.pallas import tpu as pltpu
from jax.sharding import PartitionSpec as P

HEAD_DIM = 128
SEQ_LEN = 32768
GROUP = 10
CHUNKS = 4
TILE_K = 512
MESH = pl.DeviceIdType.MESH


def rope_tables(rows, tok_dev, stride):
    half = HEAD_DIM // 2
    row = np.arange(rows)
    place = (row // tok_dev * stride + row % tok_dev).astype(np.float32)
    inverse = np.exp(
        -np.log(np.float32(1000000.0))
        * (np.float32(2.0) * np.arange(half).astype(np.float32) / np.float32(HEAD_DIM))
    ).astype(np.float32)
    angle = (place[:, None] * inverse[None, :]).astype(np.float32)
    cosine, sine = np.cos(angle).astype(np.float32), np.sin(angle).astype(np.float32)
    return np.concatenate([cosine, cosine], 1), np.concatenate([-sine, sine], 1)


def kernel(
    n,
    tok_h, gain_h, w_h, bias_h, grad_h, cos_h, sin_h,
    qkv, tg, gg_ref, bg_ref,
    tok, gain, w, bias, grad, cos, sin,
    low, part, held, run, acc, ng, scale_ref, gsend, grecv,
    in_sem, w_sem, send_sem, recv_sem, gsend_sem, grecv_sem,
):
    me = lax.axis_index("mp")
    rows, depth = tok.shape
    width = w.shape[1]
    heads = width // HEAD_DIM
    span = depth // CHUNKS
    tiles = depth // TILE_K
    per = tiles // CHUNKS
    f32 = jnp.float32

    loads = []
    for i, (src, dst) in enumerate(
        ((tok_h, tok), (gain_h, gain.at[0]), (grad_h, grad), (cos_h, cos), (sin_h, sin), (bias_h, bias.at[0]))
    ):
        c = pltpu.make_async_copy(src, dst, in_sem.at[i])
        c.start()
        loads.append(c)

    def w_copy(i):
        k = pl.ds(pl.multiple_of(i * TILE_K, TILE_K), TILE_K)
        return pltpu.make_async_copy(w_h.at[k, :], w.at[k, :], w_sem.at[i])

    @pl.loop(0, tiles)
    def _(i):
        w_copy(i).start()

    barrier = pltpu.get_barrier_semaphore()
    for k in range(1, n):
        pl.semaphore_signal(
            barrier, inc=1, device_id={"mp": lax.rem(me + k, n)}, device_id_type=MESH
        )

    def block(s):
        return pl.ds(pl.multiple_of(s * rows, rows), rows)

    def cols(c):
        return pl.ds(pl.multiple_of(c * span, span), span)

    loads[0].wait()
    loads[1].wait()
    total = jnp.zeros((rows, 1), f32)
    for c in range(CHUNKS):
        v = tok[:, c * span:(c + 1) * span].astype(f32)
        total = total + jnp.sum(v * v, axis=1, keepdims=True)
    scale = lax.rsqrt(total / depth + 1e-06)
    scale_ref[...] = jnp.broadcast_to(scale, scale_ref.shape)
    for c in range(CHUNKS):
        ks = slice(c * span, (c + 1) * span)
        held[block(me), ks] = (tok[:, ks].astype(f32) * scale * gain[:, ks]).astype(jnp.bfloat16)
    pl.semaphore_wait(barrier, n - 1)

    def transfer(way, buf, at, j, c):
        ref = buf.at[block(at), cols(c)]
        return pltpu.make_async_remote_copy(
            src_ref=ref,
            dst_ref=ref,
            send_sem=send_sem.at[way, j, c],
            recv_sem=recv_sem.at[way, j, c],
            device_id={"mp": lax.rem(me + (1 if way == 0 else n - 1), n)},
            device_id_type=MESH,
        )

    has_right, has_left = me < n - 1, me > 0

    def step(j, c):
        for way, goes, comes, back in ((0, has_right, has_left, me), (1, has_left, has_right, n - 1 - me)):
            @pl.when(comes)
            def _():
                transfer(way, held, 0, j - 1, c).wait_recv()

            @pl.when(goes)
            def _():
                @pl.when(j <= back)
                def _():
                    transfer(way, held, me - j if way == 0 else me + j, j, c).start()

                @pl.when(j > back)
                def _():
                    t = n - j + me if way == 0 else j - n + me
                    slot = t + 1 if way == 0 else t

                    @pl.when(comes)
                    def _():
                        value = part[block(t), cols(c)] + run[block(slot), cols(c)].astype(f32)
                        run[block(slot), cols(c)] = value.astype(jnp.bfloat16)

                    @pl.when(jnp.logical_not(comes))
                    def _():
                        run[block(slot), cols(c)] = part[block(t), cols(c)].astype(jnp.bfloat16)

                    transfer(way, run, slot, j, c).start()

    for c in range(CHUNKS):
        for way, goes in ((0, has_right), (1, has_left)):
            @pl.when(goes)
            def _():
                transfer(way, held, me, 0, c).start()

    for l in loads[2:]:
        l.wait()
    for h in range(heads):
        hs = slice(h * HEAD_DIM, (h + 1) * HEAD_DIM)
        x = grad[:, hs].astype(f32)
        turned = x * cos[...] - pltpu.roll(x, HEAD_DIM // 2, 1) * sin[...]
        plain = lax.rem(me * heads + h, GROUP) == GROUP - 1
        x = jnp.where(plain, x, turned)
        bg_ref[:, hs] = jnp.sum(x, axis=0, keepdims=True)
        low[:, hs] = x.astype(jnp.bfloat16)

    def backward(c):
        @pl.loop(0, per)
        def _(i):
            at = c * per + i
            w_copy(at).wait()
            k = pl.ds(pl.multiple_of(at * TILE_K, TILE_K), TILE_K)
            part[:, k] = lax.dot_general(
                low[...], w[k, :], (((1,), (1,)), ((), ())), preferred_element_type=f32
            )

    @pl.loop(0, CHUNKS)
    def _(c):
        backward(c)

        @pl.when(c > 0)
        def _():
            step(1, c - 1)

    step(1, CHUNKS - 1)

    @pl.loop(2, n - 1)
    def _(j):
        @pl.loop(0, CHUNKS)
        def _(c):
            step(j, c)

    tile_n = 640 if width % 640 == 0 else HEAD_DIM
    tiles_n = width // tile_n

    @pl.loop(0, CHUNKS)
    def _(c):
        step(n - 1, c)

        @pl.loop(0, tiles_n)
        def _(i):
            ns = pl.ds(pl.multiple_of(i * tile_n, tile_n), tile_n)
            value = jnp.dot(held[:, cols(c)], w[cols(c), ns], preferred_element_type=f32)

            @pl.when(c == 0)
            def _():
                acc[:, ns] = value

            @pl.when(c > 0)
            def _():
                acc[:, ns] += value

    for h in range(heads):
        hs = slice(h * HEAD_DIM, (h + 1) * HEAD_DIM)
        x = acc[:, hs] + bias[:, hs]
        turned = x * cos[...] + pltpu.roll(x, HEAD_DIM // 2, 1) * sin[...]
        plain = lax.rem(me * heads + h, GROUP) == GROUP - 1
        qkv[:, hs] = jnp.where(plain, x, turned).astype(jnp.bfloat16)

    def gain_copy(k, c):
        return pltpu.make_async_remote_copy(
            src_ref=gsend.at[c],
            dst_ref=grecv.at[k - 1, c],
            send_sem=gsend_sem.at[k - 1, c],
            recv_sem=grecv_sem.at[k - 1, c],
            device_id={"mp": lax.rem(me + k, n)},
            device_id_type=MESH,
        )

    scale = scale_ref[:, :1]
    inner = jnp.zeros((rows, 1), f32)
    piece = span // 8
    for c in range(CHUNKS):
        ks = slice(c * span, (c + 1) * span)
        ng[:, ks] = part[block(me), ks]
        for way, comes, slot in ((0, has_left, me + 1), (1, has_right, me)):
            @pl.when(comes)
            def _():
                transfer(way, run, slot, n - 1, c).wait_recv()
                ng[:, ks] += run[block(slot), ks].astype(f32)

        product = ng[:, ks] * tok[:, ks].astype(f32)
        gg = jnp.sum(product * scale, axis=0, keepdims=True)
        inner = inner + jnp.sum(product * gain[:, ks], axis=1, keepdims=True)
        for i in range(8):
            gsend[c, i:i + 1, :] = gg[:, i * piece:(i + 1) * piece]
        for k in range(1, n):
            gain_copy(k, c).start()

    weight = scale * scale * scale * (inner / depth)
    for c in range(CHUNKS):
        ks = slice(c * span, (c + 1) * span)
        tg[:, ks] = scale * gain[:, ks] * ng[:, ks] - tok[:, ks].astype(f32) * weight

    for c in range(CHUNKS):
        total = gsend[c]
        for k in range(1, n):
            gain_copy(k, c).wait_recv()
            total = total + grecv[k - 1, c]
        for i in range(8):
            at = c * span + i * piece
            gg_ref[:, at:at + piece] = total[i:i + 1, :]

    @pl.loop(0, n)
    def _(j):
        @pl.loop(0, CHUNKS)
        def _(c):
            for way, goes in ((0, has_right), (1, has_left)):
                @pl.when(goes)
                def _():
                    transfer(way, held, 0, j, c).wait_send()

    for c in range(CHUNKS):
        for k in range(1, n):
            gain_copy(k, c).wait_send()


def finish(qkv, tg, gg, bg, qkv_h, tg_h, gg_h, bg_h, sem):
    moves = ((qkv, qkv_h), (tg, tg_h), (gg.at[0], gg_h), (bg.at[0], bg_h))
    copies = [pltpu.make_async_copy(src, dst, sem.at[i]) for i, (src, dst) in enumerate(moves)]
    for c in copies:
        c.start()
    for c in copies:
        c.wait()


def shards(n, tokens, norm_gain, qkv_weight, qkv_bias, qkv_grad):
    rows, depth = tokens.shape
    every, width = qkv_grad.shape
    cosine, sine = rope_tables(every, rows, SEQ_LEN // n)
    bf16, f32 = jnp.bfloat16, jnp.float32
    span = depth // CHUNKS
    dma = pltpu.SemaphoreType.DMA
    hbm = pl.BlockSpec(memory_space=pl.ANY)
    vmem = pl.BlockSpec(memory_space=pltpu.VMEM)
    results = pl.pallas_call(
        functools.partial(kernel, n),
        out_shape=(
            pltpu.VMEM((every, width), bf16),
            pltpu.VMEM((rows, depth), f32),
            pltpu.VMEM((1, depth), f32),
            pltpu.VMEM((1, width), f32),
        ),
        in_specs=[hbm] * 7,
        out_specs=[vmem] * 4,
        scratch_shapes=[
            pltpu.VMEM((rows, depth), bf16),
            pltpu.VMEM((1, depth), f32),
            pltpu.VMEM((depth, width), bf16),
            pltpu.VMEM((1, width), f32),
            pltpu.VMEM((every, width), bf16),
            pltpu.VMEM((every, HEAD_DIM), f32),
            pltpu.VMEM((every, HEAD_DIM), f32),
            pltpu.VMEM((every, width), bf16),
            pltpu.VMEM((every, depth), f32),
            pltpu.VMEM((every, depth), bf16),
            pltpu.VMEM((every + rows, depth), bf16),
            pltpu.VMEM((every, width), f32),
            pltpu.VMEM((rows, depth), f32),
            pltpu.VMEM((rows, HEAD_DIM), f32),
            pltpu.VMEM((CHUNKS, 8, span // 8), f32),
            pltpu.VMEM((n - 1, CHUNKS, 8, span // 8), f32),
            dma((6,)),
            dma((depth // TILE_K,)),
            dma((2, n, CHUNKS)),
            dma((2, n, CHUNKS)),
            dma((n - 1, CHUNKS)),
            dma((n - 1, CHUNKS)),
        ],
        compiler_params=pltpu.CompilerParams(
            collective_id=0, has_side_effects=True, vmem_limit_bytes=60000000
        ),
        cost_estimate=pl.CostEstimate(
            flops=4 * every * depth * width, bytes_accessed=2 * depth * width, transcendentals=0
        ),
    )(
        tokens, norm_gain, qkv_weight, qkv_bias, qkv_grad,
        jnp.asarray(cosine), jnp.asarray(sine),
    )
    return pl.pallas_call(
        finish,
        out_shape=(
            jax.ShapeDtypeStruct((every, width), bf16),
            jax.ShapeDtypeStruct((rows, depth), f32),
            jax.ShapeDtypeStruct((depth,), f32),
            jax.ShapeDtypeStruct((width,), f32),
        ),
        in_specs=[vmem] * 4,
        out_specs=[hbm] * 4,
        scratch_shapes=[dma((4,))],
        compiler_params=pltpu.CompilerParams(vmem_limit_bytes=1 << 20),
    )(*results)


def solution(mesh):
    in_specs = (P(("dp", "mp"), None), P(), P(None, "mp"), P("mp"), P("dp", "mp"))
    out_specs = (P("dp", "mp"), P(("dp", "mp"), None), P("dp"), P(("dp", "mp")))
    body = functools.partial(shards, mesh.shape["mp"])
    return jax.shard_map(body, mesh=mesh, in_specs=in_specs, out_specs=out_specs, check_vma=False)
```

```python
import functools

import jax
import jax.numpy as jnp
import numpy as np
from jax import lax
from jax.experimental import pallas as pl
from jax.experimental.pallas import tpu as pltpu
from jax.sharding import PartitionSpec as P

HEAD_DIM = 128
SEQ_LEN = 32768
GROUP = 10
CHUNKS = 4
TILE_K = 512
MESH = pl.DeviceIdType.MESH


def rope_tables(rows, tok_dev, stride):
    half = HEAD_DIM // 2
    row = np.arange(rows)
    place = (row // tok_dev * stride + row % tok_dev).astype(np.float32)
    inverse = np.exp(
        -np.log(np.float32(1000000.0))
        * (np.float32(2.0) * np.arange(half).astype(np.float32) / np.float32(HEAD_DIM))
    ).astype(np.float32)
    angle = (place[:, None] * inverse[None, :]).astype(np.float32)
    cosine, sine = np.cos(angle).astype(np.float32), np.sin(angle).astype(np.float32)
    return np.concatenate([cosine, cosine], 1), np.concatenate([-sine, sine], 1)


def kernel(
    n,
    tok_h, gain_h, w_h, bias_h, grad_h, cos_h, sin_h,
    qkv, tg, gg_ref, bg_ref,
    tok, gain, w, bias, grad, cos, sin,
    low, part, held, run, acc, ng, scale_ref, gmine, gsend, grecv,
    in_sem, w_sem, send_sem, recv_sem, gsend_sem, grecv_sem,
):
    me = lax.axis_index("mp")
    rows, depth = tok.shape
    width = w.shape[1]
    heads = width // HEAD_DIM
    span = depth // CHUNKS
    tiles = depth // TILE_K
    per = tiles // CHUNKS
    f32 = jnp.float32

    has_right, has_left = me < n - 1, me > 0
    barrier = pltpu.get_barrier_semaphore()
    for there, k in ((has_right, 1), (has_left, n - 1)):
        @pl.when(there)
        def _():
            pl.semaphore_signal(
                barrier, inc=1, device_id={"mp": lax.rem(me + k, n)}, device_id_type=MESH
            )

    loads = []
    for i, (src, dst) in enumerate(
        ((tok_h, tok), (gain_h, gain.at[0]), (grad_h, grad), (cos_h, cos), (sin_h, sin), (bias_h, bias.at[0]))
    ):
        c = pltpu.make_async_copy(src, dst, in_sem.at[i])
        c.start()
        loads.append(c)

    def w_copy(i):
        k = pl.ds(pl.multiple_of(i * TILE_K, TILE_K), TILE_K)
        return pltpu.make_async_copy(w_h.at[k, :], w.at[k, :], w_sem.at[i])

    def block(s):
        return pl.ds(pl.multiple_of(s * rows, rows), rows)

    def cols(c):
        return pl.ds(pl.multiple_of(c * span, span), span)

    loads[0].wait()
    loads[1].wait()
    total = jnp.zeros((rows, 1), f32)
    for c in range(CHUNKS):
        v = tok[:, c * span:(c + 1) * span].astype(f32)
        total = total + jnp.sum(v * v, axis=1, keepdims=True)
    scale = lax.rsqrt(total / depth + 1e-06)
    scale_ref[...] = jnp.broadcast_to(scale, scale_ref.shape)
    for c in range(CHUNKS):
        ks = slice(c * span, (c + 1) * span)
        held[block(me), ks] = (tok[:, ks].astype(f32) * scale * gain[:, ks]).astype(jnp.bfloat16)
    inside = has_right & has_left

    @pl.when(inside)
    def _():
        pl.semaphore_wait(barrier, 2)

    @pl.when(jnp.logical_not(inside))
    def _():
        pl.semaphore_wait(barrier, 1)


    def transfer(way, buf, at, j, c):
        ref = buf.at[block(at), cols(c)]
        return pltpu.make_async_remote_copy(
            src_ref=ref,
            dst_ref=ref,
            send_sem=send_sem.at[way, j, c],
            recv_sem=recv_sem.at[way, j, c],
            device_id={"mp": lax.rem(me + (1 if way == 0 else n - 1), n)},
            device_id_type=MESH,
        )

    def step(j, c):
        for way, goes, comes, back in ((0, has_right, has_left, me), (1, has_left, has_right, n - 1 - me)):
            @pl.when(comes)
            def _():
                transfer(way, held, 0, j - 1, c).wait_recv()

            @pl.when(goes)
            def _():
                @pl.when(j <= back)
                def _():
                    transfer(way, held, me - j if way == 0 else me + j, j, c).start()

                @pl.when(j > back)
                def _():
                    t = n - j + me if way == 0 else j - n + me
                    slot = t + 1 if way == 0 else t

                    @pl.when(comes)
                    def _():
                        value = part[block(t), cols(c)] + run[block(slot), cols(c)].astype(f32)
                        run[block(slot), cols(c)] = value.astype(jnp.bfloat16)

                    @pl.when(jnp.logical_not(comes))
                    def _():
                        run[block(slot), cols(c)] = part[block(t), cols(c)].astype(jnp.bfloat16)

                    transfer(way, run, slot, j, c).start()

    for c in range(CHUNKS):
        for way, goes in ((0, has_right), (1, has_left)):
            @pl.when(goes)
            def _():
                transfer(way, held, me, 0, c).start()

    @pl.loop(0, tiles)
    def _(i):
        w_copy(i).start()

    for l in loads[2:]:
        l.wait()
    for h in range(heads):
        hs = slice(h * HEAD_DIM, (h + 1) * HEAD_DIM)
        x = grad[:, hs].astype(f32)
        turned = x * cos[...] - pltpu.roll(x, HEAD_DIM // 2, 1) * sin[...]
        plain = lax.rem(me * heads + h, GROUP) == GROUP - 1
        x = jnp.where(plain, x, turned)
        bg_ref[:, hs] = jnp.sum(x, axis=0, keepdims=True)
        low[:, hs] = x.astype(jnp.bfloat16)

    def backward(c):
        @pl.loop(0, per)
        def _(i):
            at = c * per + i
            w_copy(at).wait()
            k = pl.ds(pl.multiple_of(at * TILE_K, TILE_K), TILE_K)
            part[:, k] = lax.dot_general(
                low[...], w[k, :], (((1,), (1,)), ((), ())), preferred_element_type=f32
            )

    @pl.loop(0, CHUNKS)
    def _(c):
        backward(c)

        @pl.when(c > 0)
        def _():
            step(1, c - 1)

    step(1, CHUNKS - 1)

    @pl.loop(2, n - 1)
    def _(j):
        @pl.loop(0, CHUNKS)
        def _(c):
            step(j, c)

    tile_n = 640 if width % 640 == 0 else HEAD_DIM
    tiles_n = width // tile_n

    def gain_copy(k, c):
        return pltpu.make_async_remote_copy(
            src_ref=gsend.at[c],
            dst_ref=grecv.at[k - 1, c],
            send_sem=gsend_sem.at[k - 1, c],
            recv_sem=grecv_sem.at[k - 1, c],
            device_id={"mp": lax.rem(me + k, n)},
            device_id_type=MESH,
        )

    piece = span // 16

    @pl.loop(0, CHUNKS)
    def _(c):
        step(n - 1, c)
        for i in range(16):
            ks = pl.ds(pl.multiple_of(c * span + i * piece, piece), piece)
            share = jnp.sum(part[:, ks] * held[:, ks].astype(f32), axis=0, keepdims=True)
            gmine[c, i:i + 1, :] = share / gain[:, ks]
        gsend[c] = gmine[c].astype(jnp.bfloat16)

        @pl.loop(0, tiles_n)
        def _(i):
            ns = pl.ds(pl.multiple_of(i * tile_n, tile_n), tile_n)
            value = jnp.dot(held[:, cols(c)], w[cols(c), ns], preferred_element_type=f32)

            @pl.when(c == 0)
            def _():
                acc[:, ns] = value

            @pl.when(c > 0)
            def _():
                acc[:, ns] += value

            @pl.when(i == 0)
            def _():
                for k in range(1, n):
                    gain_copy(k, c).start()

    for h in range(heads):
        hs = slice(h * HEAD_DIM, (h + 1) * HEAD_DIM)
        x = acc[:, hs] + bias[:, hs]
        turned = x * cos[...] + pltpu.roll(x, HEAD_DIM // 2, 1) * sin[...]
        plain = lax.rem(me * heads + h, GROUP) == GROUP - 1
        qkv[:, hs] = jnp.where(plain, x, turned).astype(jnp.bfloat16)

    scale = scale_ref[:, :1]
    inner = jnp.zeros((rows, 1), f32)
    for c in range(CHUNKS):
        ks = slice(c * span, (c + 1) * span)
        ng[:, ks] = part[block(me), ks]
        for way, comes, slot in ((0, has_left, me + 1), (1, has_right, me)):
            @pl.when(comes)
            def _():
                transfer(way, run, slot, n - 1, c).wait_recv()
                ng[:, ks] += run[block(slot), ks].astype(f32)

        product = ng[:, ks] * tok[:, ks].astype(f32)
        inner = inner + jnp.sum(product * gain[:, ks], axis=1, keepdims=True)

    weight = scale * scale * scale * (inner / depth)
    for c in range(CHUNKS):
        ks = slice(c * span, (c + 1) * span)
        tg[:, ks] = scale * gain[:, ks] * ng[:, ks] - tok[:, ks].astype(f32) * weight

    for c in range(CHUNKS):
        total = gmine[c]
        for k in range(1, n):
            gain_copy(k, c).wait_recv()
            total = total + grecv[k - 1, c].astype(f32)
        for i in range(16):
            at = c * span + i * piece
            gg_ref[:, at:at + piece] = total[i:i + 1, :]

    @pl.loop(0, n)
    def _(j):
        @pl.loop(0, CHUNKS)
        def _(c):
            for way, goes in ((0, has_right), (1, has_left)):
                @pl.when(goes)
                def _():
                    transfer(way, held, 0, j, c).wait_send()

    for c in range(CHUNKS):
        for k in range(1, n):
            gain_copy(k, c).wait_send()


def finish(qkv, tg, gg, bg, qkv_h, tg_h, gg_h, bg_h, sem):
    moves = ((qkv, qkv_h), (tg, tg_h), (gg.at[0], gg_h), (bg.at[0], bg_h))
    copies = [pltpu.make_async_copy(src, dst, sem.at[i]) for i, (src, dst) in enumerate(moves)]
    for c in copies:
        c.start()
    for c in copies:
        c.wait()


def shards(n, tokens, norm_gain, qkv_weight, qkv_bias, qkv_grad):
    rows, depth = tokens.shape
    every, width = qkv_grad.shape
    cosine, sine = rope_tables(every, rows, SEQ_LEN // n)
    bf16, f32 = jnp.bfloat16, jnp.float32
    span = depth // CHUNKS
    dma = pltpu.SemaphoreType.DMA
    hbm = pl.BlockSpec(memory_space=pl.ANY)
    vmem = pl.BlockSpec(memory_space=pltpu.VMEM)
    results = pl.pallas_call(
        functools.partial(kernel, n),
        out_shape=(
            pltpu.VMEM((every, width), bf16),
            pltpu.VMEM((rows, depth), f32),
            pltpu.VMEM((1, depth), f32),
            pltpu.VMEM((1, width), f32),
        ),
        in_specs=[hbm] * 7,
        out_specs=[vmem] * 4,
        scratch_shapes=[
            pltpu.VMEM((rows, depth), bf16),
            pltpu.VMEM((1, depth), f32),
            pltpu.VMEM((depth, width), bf16),
            pltpu.VMEM((1, width), f32),
            pltpu.VMEM((every, width), bf16),
            pltpu.VMEM((every, HEAD_DIM), f32),
            pltpu.VMEM((every, HEAD_DIM), f32),
            pltpu.VMEM((every, width), bf16),
            pltpu.VMEM((every, depth), f32),
            pltpu.VMEM((every, depth), bf16),
            pltpu.VMEM((every + rows, depth), bf16),
            pltpu.VMEM((every, width), f32),
            pltpu.VMEM((rows, depth), f32),
            pltpu.VMEM((rows, HEAD_DIM), f32),
            pltpu.VMEM((CHUNKS, 16, span // 16), f32),
            pltpu.VMEM((CHUNKS, 16, span // 16), bf16),
            pltpu.VMEM((n - 1, CHUNKS, 16, span // 16), bf16),
            dma((6,)),
            dma((depth // TILE_K,)),
            dma((2, n, CHUNKS)),
            dma((2, n, CHUNKS)),
            dma((n - 1, CHUNKS)),
            dma((n - 1, CHUNKS)),
        ],
        compiler_params=pltpu.CompilerParams(
            collective_id=0, has_side_effects=True, vmem_limit_bytes=60000000
        ),
        cost_estimate=pl.CostEstimate(
            flops=4 * every * depth * width, bytes_accessed=2 * depth * width, transcendentals=0
        ),
    )(
        tokens, norm_gain, qkv_weight, qkv_bias, qkv_grad,
        jnp.asarray(cosine), jnp.asarray(sine),
    )
    return pl.pallas_call(
        finish,
        out_shape=(
            jax.ShapeDtypeStruct((every, width), bf16),
            jax.ShapeDtypeStruct((rows, depth), f32),
            jax.ShapeDtypeStruct((depth,), f32),
            jax.ShapeDtypeStruct((width,), f32),
        ),
        in_specs=[vmem] * 4,
        out_specs=[hbm] * 4,
        scratch_shapes=[dma((4,))],
        compiler_params=pltpu.CompilerParams(vmem_limit_bytes=1 << 20),
    )(*results)


def solution(mesh):
    in_specs = (P(("dp", "mp"), None), P(), P(None, "mp"), P("mp"), P("dp", "mp"))
    out_specs = (P("dp", "mp"), P(("dp", "mp"), None), P("dp"), P(("dp", "mp")))
    body = functools.partial(shards, mesh.shape["mp"])
    return jax.shard_map(body, mesh=mesh, in_specs=in_specs, out_specs=out_specs, check_vma=False)
```

```python
import functools

import jax
import jax.numpy as jnp
import numpy as np
from jax import lax
from jax.experimental import pallas as pl
from jax.experimental.pallas import tpu as pltpu
from jax.sharding import PartitionSpec as P

HEAD_DIM = 128
SEQ_LEN = 32768
GROUP = 10
CHUNKS = 4
TILE_K = 512
MESH = pl.DeviceIdType.MESH


def rope_tables(rows, tok_dev, stride):
    half = HEAD_DIM // 2
    row = np.arange(rows)
    place = (row // tok_dev * stride + row % tok_dev).astype(np.float32)
    inverse = np.exp(
        -np.log(np.float32(1000000.0))
        * (np.float32(2.0) * np.arange(half).astype(np.float32) / np.float32(HEAD_DIM))
    ).astype(np.float32)
    angle = (place[:, None] * inverse[None, :]).astype(np.float32)
    cosine, sine = np.cos(angle).astype(np.float32), np.sin(angle).astype(np.float32)
    return np.concatenate([cosine, cosine], 1), np.concatenate([-sine, sine], 1)


def kernel(
    n,
    tok_h, gain_h, w_h, bias_h, grad_h, cos_h, sin_h,
    qkv, tg, gg_ref, bg_ref,
    tok, gain, w, bias, grad, cos, sin,
    low, part, held, run, acc, ng, scale_ref, gmine, gsend, grecv,
    in_sem, w_sem, send_sem, recv_sem, gsend_sem, grecv_sem,
):
    me = lax.axis_index("mp")
    rows, depth = tok.shape
    width = w.shape[1]
    heads = width // HEAD_DIM
    span = depth // CHUNKS
    tiles = depth // TILE_K
    per = tiles // CHUNKS
    f32 = jnp.float32

    has_right, has_left = me < n - 1, me > 0
    barrier = pltpu.get_barrier_semaphore()
    for there, k in ((has_right, 1), (has_left, n - 1)):
        @pl.when(there)
        def _():
            pl.semaphore_signal(
                barrier, inc=1, device_id={"mp": lax.rem(me + k, n)}, device_id_type=MESH
            )

    loads = []
    for i, (src, dst) in enumerate(
        ((tok_h, tok), (gain_h, gain.at[0]), (grad_h, grad), (cos_h, cos), (sin_h, sin), (bias_h, bias.at[0]))
    ):
        c = pltpu.make_async_copy(src, dst, in_sem.at[i])
        c.start()
        loads.append(c)

    def w_copy(i):
        k = pl.ds(pl.multiple_of(i * TILE_K, TILE_K), TILE_K)
        return pltpu.make_async_copy(w_h.at[k, :], w.at[k, :], w_sem.at[i])

    def block(s):
        return pl.ds(pl.multiple_of(s * rows, rows), rows)

    def cols(c):
        return pl.ds(pl.multiple_of(c * span, span), span)

    loads[0].wait()
    loads[1].wait()
    total = jnp.zeros((rows, 1), f32)
    for c in range(CHUNKS):
        v = tok[:, c * span:(c + 1) * span].astype(f32)
        total = total + jnp.sum(v * v, axis=1, keepdims=True)
    scale = lax.rsqrt(total / depth + 1e-06)
    scale_ref[...] = jnp.broadcast_to(scale, scale_ref.shape)
    for c in range(CHUNKS):
        ks = slice(c * span, (c + 1) * span)
        held[block(me), ks] = (tok[:, ks].astype(f32) * scale * gain[:, ks]).astype(jnp.bfloat16)
    inside = has_right & has_left

    @pl.when(inside)
    def _():
        pl.semaphore_wait(barrier, 2)

    @pl.when(jnp.logical_not(inside))
    def _():
        pl.semaphore_wait(barrier, 1)


    def transfer(way, buf, at, j, c):
        ref = buf.at[block(at), cols(c)]
        return pltpu.make_async_remote_copy(
            src_ref=ref,
            dst_ref=ref,
            send_sem=send_sem.at[way, j, c],
            recv_sem=recv_sem.at[way, j, c],
            device_id={"mp": lax.rem(me + (1 if way == 0 else n - 1), n)},
            device_id_type=MESH,
        )

    def arrive(j, c):
        for way, comes in ((0, has_left), (1, has_right)):
            @pl.when(comes)
            def _():
                transfer(way, held, 0, j - 1, c).wait_recv()

    def depart(j, c):
        for way, goes, comes, back in ((0, has_right, has_left, me), (1, has_left, has_right, n - 1 - me)):
            @pl.when(goes)
            def _():
                @pl.when(j <= back)
                def _():
                    transfer(way, held, me - j if way == 0 else me + j, j, c).start()

                @pl.when(j > back)
                def _():
                    t = n - j + me if way == 0 else j - n + me
                    slot = t + 1 if way == 0 else t

                    @pl.when(comes)
                    def _():
                        value = part[block(t), cols(c)] + run[block(slot), cols(c)].astype(f32)
                        run[block(slot), cols(c)] = value.astype(jnp.bfloat16)

                    @pl.when(jnp.logical_not(comes))
                    def _():
                        run[block(slot), cols(c)] = part[block(t), cols(c)].astype(jnp.bfloat16)

                    transfer(way, run, slot, j, c).start()

    def step(j, c):
        arrive(j, c)
        depart(j, c)

    for c in range(CHUNKS):
        for way, goes in ((0, has_right), (1, has_left)):
            @pl.when(goes)
            def _():
                transfer(way, held, me, 0, c).start()

    @pl.loop(0, tiles)
    def _(i):
        w_copy(i).start()

    for l in loads[2:]:
        l.wait()
    for h in range(heads):
        hs = slice(h * HEAD_DIM, (h + 1) * HEAD_DIM)
        x = grad[:, hs].astype(f32)
        turned = x * cos[...] - pltpu.roll(x, HEAD_DIM // 2, 1) * sin[...]
        plain = lax.rem(me * heads + h, GROUP) == GROUP - 1
        x = jnp.where(plain, x, turned)
        bg_ref[:, hs] = jnp.sum(x, axis=0, keepdims=True)
        low[:, hs] = x.astype(jnp.bfloat16)

    def backward(c):
        @pl.loop(0, per)
        def _(i):
            at = c * per + i
            w_copy(at).wait()
            k = pl.ds(pl.multiple_of(at * TILE_K, TILE_K), TILE_K)
            part[:, k] = lax.dot_general(
                low[...], w[k, :], (((1,), (1,)), ((), ())), preferred_element_type=f32
            )

    @pl.loop(0, CHUNKS)
    def _(c):
        backward(c)

        @pl.when(c > 0)
        def _():
            step(1, c - 1)

    step(1, CHUNKS - 1)

    @pl.loop(2, n - 1)
    def _(j):
        @pl.loop(0, CHUNKS)
        def _(c):
            step(j, c)

    tile_n = 640 if width % 640 == 0 else HEAD_DIM
    tiles_n = width // tile_n

    def gain_copy(k):
        return pltpu.make_async_remote_copy(
            src_ref=gsend,
            dst_ref=grecv.at[k - 1],
            send_sem=gsend_sem.at[k - 1],
            recv_sem=grecv_sem.at[k - 1],
            device_id={"mp": lax.rem(me + k, n)},
            device_id_type=MESH,
        )

    piece = span // 16

    @pl.loop(0, CHUNKS)
    def _(c):
        arrive(n - 1, c)
        for i in range(16):
            ks = pl.ds(pl.multiple_of(c * span + i * piece, piece), piece)
            share = jnp.sum(part[:, ks] * held[:, ks].astype(f32), axis=0, keepdims=True)
            gmine[c, i:i + 1, :] = share / gain[:, ks]
        gsend[c] = gmine[c].astype(jnp.bfloat16)

        @pl.when(c == CHUNKS - 1)
        def _():
            for k in range(1, n):
                gain_copy(k).start()

        depart(n - 1, c)

        @pl.loop(0, tiles_n)
        def _(i):
            ns = pl.ds(pl.multiple_of(i * tile_n, tile_n), tile_n)
            value = jnp.dot(held[:, cols(c)], w[cols(c), ns], preferred_element_type=f32)

            @pl.when(c == 0)
            def _():
                acc[:, ns] = value

            @pl.when(c > 0)
            def _():
                acc[:, ns] += value

    for h in range(heads):
        hs = slice(h * HEAD_DIM, (h + 1) * HEAD_DIM)
        x = acc[:, hs] + bias[:, hs]
        turned = x * cos[...] + pltpu.roll(x, HEAD_DIM // 2, 1) * sin[...]
        plain = lax.rem(me * heads + h, GROUP) == GROUP - 1
        qkv[:, hs] = jnp.where(plain, x, turned).astype(jnp.bfloat16)

    scale = scale_ref[:, :1]
    inner = jnp.zeros((rows, 1), f32)
    for c in range(CHUNKS):
        ks = slice(c * span, (c + 1) * span)
        ng[:, ks] = part[block(me), ks]
        for way, comes, slot in ((0, has_left, me + 1), (1, has_right, me)):
            @pl.when(comes)
            def _():
                transfer(way, run, slot, n - 1, c).wait_recv()
                ng[:, ks] += run[block(slot), ks].astype(f32)

        product = ng[:, ks] * tok[:, ks].astype(f32)
        inner = inner + jnp.sum(product * gain[:, ks], axis=1, keepdims=True)

    weight = scale * scale * scale * (inner / depth)
    for c in range(CHUNKS):
        ks = slice(c * span, (c + 1) * span)
        tg[:, ks] = scale * gain[:, ks] * ng[:, ks] - tok[:, ks].astype(f32) * weight

    for k in range(1, n):
        gain_copy(k).wait_recv()
    for c in range(CHUNKS):
        total = gmine[c]
        for k in range(1, n):
            total = total + grecv[k - 1, c].astype(f32)
        for i in range(16):
            at = c * span + i * piece
            gg_ref[:, at:at + piece] = total[i:i + 1, :]

    @pl.loop(0, n)
    def _(j):
        @pl.loop(0, CHUNKS)
        def _(c):
            for way, goes in ((0, has_right), (1, has_left)):
                @pl.when(goes)
                def _():
                    transfer(way, held, 0, j, c).wait_send()

    for k in range(1, n):
        gain_copy(k).wait_send()


def finish(qkv, tg, gg, bg, qkv_h, tg_h, gg_h, bg_h, sem):
    moves = ((qkv, qkv_h), (tg, tg_h), (gg.at[0], gg_h), (bg.at[0], bg_h))
    copies = [pltpu.make_async_copy(src, dst, sem.at[i]) for i, (src, dst) in enumerate(moves)]
    for c in copies:
        c.start()
    for c in copies:
        c.wait()


def shards(n, tokens, norm_gain, qkv_weight, qkv_bias, qkv_grad):
    rows, depth = tokens.shape
    every, width = qkv_grad.shape
    cosine, sine = rope_tables(every, rows, SEQ_LEN // n)
    bf16, f32 = jnp.bfloat16, jnp.float32
    span = depth // CHUNKS
    dma = pltpu.SemaphoreType.DMA
    hbm = pl.BlockSpec(memory_space=pl.ANY)
    vmem = pl.BlockSpec(memory_space=pltpu.VMEM)
    results = pl.pallas_call(
        functools.partial(kernel, n),
        out_shape=(
            pltpu.VMEM((every, width), bf16),
            pltpu.VMEM((rows, depth), f32),
            pltpu.VMEM((1, depth), f32),
            pltpu.VMEM((1, width), f32),
        ),
        in_specs=[hbm] * 7,
        out_specs=[vmem] * 4,
        scratch_shapes=[
            pltpu.VMEM((rows, depth), bf16),
            pltpu.VMEM((1, depth), f32),
            pltpu.VMEM((depth, width), bf16),
            pltpu.VMEM((1, width), f32),
            pltpu.VMEM((every, width), bf16),
            pltpu.VMEM((every, HEAD_DIM), f32),
            pltpu.VMEM((every, HEAD_DIM), f32),
            pltpu.VMEM((every, width), bf16),
            pltpu.VMEM((every, depth), f32),
            pltpu.VMEM((every, depth), bf16),
            pltpu.VMEM((every + rows, depth), bf16),
            pltpu.VMEM((every, width), f32),
            pltpu.VMEM((rows, depth), f32),
            pltpu.VMEM((rows, HEAD_DIM), f32),
            pltpu.VMEM((CHUNKS, 16, span // 16), f32),
            pltpu.VMEM((CHUNKS, 16, span // 16), bf16),
            pltpu.VMEM((n - 1, CHUNKS, 16, span // 16), bf16),
            dma((6,)),
            dma((depth // TILE_K,)),
            dma((2, n, CHUNKS)),
            dma((2, n, CHUNKS)),
            dma((n - 1,)),
            dma((n - 1,)),
        ],
        compiler_params=pltpu.CompilerParams(
            collective_id=0, has_side_effects=True, vmem_limit_bytes=60000000
        ),
        cost_estimate=pl.CostEstimate(
            flops=4 * every * depth * width, bytes_accessed=2 * depth * width, transcendentals=0
        ),
    )(
        tokens, norm_gain, qkv_weight, qkv_bias, qkv_grad,
        jnp.asarray(cosine), jnp.asarray(sine),
    )
    return pl.pallas_call(
        finish,
        out_shape=(
            jax.ShapeDtypeStruct((every, width), bf16),
            jax.ShapeDtypeStruct((rows, depth), f32),
            jax.ShapeDtypeStruct((depth,), f32),
            jax.ShapeDtypeStruct((width,), f32),
        ),
        in_specs=[vmem] * 4,
        out_specs=[hbm] * 4,
        scratch_shapes=[dma((4,))],
        compiler_params=pltpu.CompilerParams(vmem_limit_bytes=1 << 20),
    )(*results)


def solution(mesh):
    in_specs = (P(("dp", "mp"), None), P(), P(None, "mp"), P("mp"), P("dp", "mp"))
    out_specs = (P("dp", "mp"), P(("dp", "mp"), None), P("dp"), P(("dp", "mp")))
    body = functools.partial(shards, mesh.shape["mp"])
    return jax.shard_map(body, mesh=mesh, in_specs=in_specs, out_specs=out_specs, check_vma=False)
```

```python
import functools

import jax
import jax.numpy as jnp
import numpy as np
from jax import lax
from jax.experimental import pallas as pl
from jax.experimental.pallas import tpu as pltpu
from jax.sharding import PartitionSpec as P

HEAD_DIM = 128
SEQ_LEN = 32768
GROUP = 10
CHUNKS = 4
TILE_K = 512
MESH = pl.DeviceIdType.MESH


def rope_tables(rows, tok_dev, stride):
    half = HEAD_DIM // 2
    row = np.arange(rows)
    place = (row // tok_dev * stride + row % tok_dev).astype(np.float32)
    inverse = np.exp(
        -np.log(np.float32(1000000.0))
        * (np.float32(2.0) * np.arange(half).astype(np.float32) / np.float32(HEAD_DIM))
    ).astype(np.float32)
    angle = (place[:, None] * inverse[None, :]).astype(np.float32)
    cosine, sine = np.cos(angle).astype(np.float32), np.sin(angle).astype(np.float32)
    return np.concatenate([cosine, cosine], 1), np.concatenate([-sine, sine], 1)


def kernel(
    n,
    tok_h, gain_h, w_h, bias_h, grad_h, cos_h, sin_h,
    qkv, tg, gg_ref, bg_ref,
    tok, gain, w, bias, grad, cos, sin,
    low, part, held, run, acc, ng, scale_ref, gmine, gsend, grecv,
    in_sem, w_sem, send_sem, recv_sem, gsend_sem, grecv_sem,
):
    me = lax.axis_index("mp")
    rows, depth = tok.shape
    width = w.shape[1]
    heads = width // HEAD_DIM
    span = depth // CHUNKS
    tiles = depth // TILE_K
    per = tiles // CHUNKS
    f32 = jnp.float32

    has_right, has_left = me < n - 1, me > 0
    barrier = pltpu.get_barrier_semaphore()
    for there, k in ((has_right, 1), (has_left, n - 1)):
        @pl.when(there)
        def _():
            pl.semaphore_signal(
                barrier, inc=1, device_id={"mp": lax.rem(me + k, n)}, device_id_type=MESH
            )

    loads = []
    for i, (src, dst) in enumerate(
        ((tok_h, tok), (gain_h, gain.at[0]), (grad_h, grad), (cos_h, cos), (sin_h, sin), (bias_h, bias.at[0]))
    ):
        c = pltpu.make_async_copy(src, dst, in_sem.at[i])
        c.start()
        loads.append(c)

    def w_copy(i):
        k = pl.ds(pl.multiple_of(i * TILE_K, TILE_K), TILE_K)
        return pltpu.make_async_copy(w_h.at[k, :], w.at[k, :], w_sem.at[i])

    def block(s):
        return pl.ds(pl.multiple_of(s * rows, rows), rows)

    def cols(c):
        return pl.ds(pl.multiple_of(c * span, span), span)

    loads[0].wait()
    loads[1].wait()
    total = jnp.zeros((rows, 1), f32)
    for c in range(CHUNKS):
        v = tok[:, c * span:(c + 1) * span].astype(f32)
        total = total + jnp.sum(v * v, axis=1, keepdims=True)
    scale = lax.rsqrt(total / depth + 1e-06)
    scale_ref[...] = jnp.broadcast_to(scale, scale_ref.shape)
    for c in range(CHUNKS):
        ks = slice(c * span, (c + 1) * span)
        held[block(me), ks] = (tok[:, ks].astype(f32) * scale * gain[:, ks]).astype(jnp.bfloat16)
    inside = has_right & has_left

    @pl.when(inside)
    def _():
        pl.semaphore_wait(barrier, 2)

    @pl.when(jnp.logical_not(inside))
    def _():
        pl.semaphore_wait(barrier, 1)


    def transfer(way, buf, at, j, c):
        ref = buf.at[block(at), cols(c)]
        return pltpu.make_async_remote_copy(
            src_ref=ref,
            dst_ref=ref,
            send_sem=send_sem.at[way, j, c],
            recv_sem=recv_sem.at[way, j, c],
            device_id={"mp": lax.rem(me + (1 if way == 0 else n - 1), n)},
            device_id_type=MESH,
        )

    def arrive(j, c):
        for way, comes in ((0, has_left), (1, has_right)):
            @pl.when(comes)
            def _():
                transfer(way, held, 0, j - 1, c).wait_recv()

    def depart(j, c):
        for way, goes, comes, back in ((0, has_right, has_left, me), (1, has_left, has_right, n - 1 - me)):
            @pl.when(goes)
            def _():
                @pl.when(j <= back)
                def _():
                    transfer(way, held, me - j if way == 0 else me + j, j, c).start()

                @pl.when(j > back)
                def _():
                    t = n - j + me if way == 0 else j - n + me
                    slot = t + 1 if way == 0 else t

                    @pl.when(comes)
                    def _():
                        value = part[block(t), cols(c)] + run[block(slot), cols(c)].astype(f32)
                        run[block(slot), cols(c)] = value.astype(jnp.bfloat16)

                    @pl.when(jnp.logical_not(comes))
                    def _():
                        run[block(slot), cols(c)] = part[block(t), cols(c)].astype(jnp.bfloat16)

                    transfer(way, run, slot, j, c).start()

    def step(j, c):
        arrive(j, c)
        depart(j, c)

    for c in range(CHUNKS):
        for way, goes in ((0, has_right), (1, has_left)):
            @pl.when(goes)
            def _():
                transfer(way, held, me, 0, c).start()

    @pl.loop(0, tiles)
    def _(i):
        w_copy(i).start()

    for l in loads[2:]:
        l.wait()
    for h in range(heads):
        hs = slice(h * HEAD_DIM, (h + 1) * HEAD_DIM)
        x = grad[:, hs].astype(f32)
        turned = x * cos[...] - pltpu.roll(x, HEAD_DIM // 2, 1) * sin[...]
        plain = lax.rem(me * heads + h, GROUP) == GROUP - 1
        x = jnp.where(plain, x, turned)
        bg_ref[:, hs] = jnp.sum(x, axis=0, keepdims=True)
        low[:, hs] = x.astype(jnp.bfloat16)

    def backward(c):
        @pl.loop(0, per)
        def _(i):
            at = c * per + i
            w_copy(at).wait()
            k = pl.ds(pl.multiple_of(at * TILE_K, TILE_K), TILE_K)
            part[:, k] = lax.dot_general(
                low[...], w[k, :], (((1,), (1,)), ((), ())), preferred_element_type=f32
            )

    @pl.loop(0, CHUNKS)
    def _(c):
        backward(c)

        @pl.when(c > 0)
        def _():
            step(1, c - 1)

    step(1, CHUNKS - 1)

    @pl.loop(2, n - 1)
    def _(j):
        @pl.loop(0, CHUNKS)
        def _(c):
            step(j, c)

    tile_n = 640 if width % 640 == 0 else HEAD_DIM
    tiles_n = width // tile_n

    def gain_copy(k):
        return pltpu.make_async_remote_copy(
            src_ref=gsend,
            dst_ref=grecv.at[k - 1],
            send_sem=gsend_sem.at[k - 1],
            recv_sem=grecv_sem.at[k - 1],
            device_id={"mp": lax.rem(me + k, n)},
            device_id_type=MESH,
        )

    piece = span // 16

    @pl.loop(0, CHUNKS)
    def _(c):
        arrive(n - 1, c)
        for i in range(16):
            ks = pl.ds(pl.multiple_of(c * span + i * piece, piece), piece)
            share = jnp.sum(part[:, ks] * held[:, ks].astype(f32), axis=0, keepdims=True)
            gmine[c, i:i + 1, :] = share / gain[:, ks]
        gsend[c] = gmine[c].astype(jnp.bfloat16)

        @pl.when(c == CHUNKS - 1)
        def _():
            for k in range(1, n):
                gain_copy(k).start()

        depart(n - 1, c)

        @pl.loop(0, tiles_n)
        def _(i):
            ns = pl.ds(pl.multiple_of(i * tile_n, tile_n), tile_n)
            value = jnp.dot(held[:, cols(c)], w[cols(c), ns], preferred_element_type=f32)

            @pl.when(c == 0)
            def _():
                acc[:, ns] = value

            @pl.when(c > 0)
            def _():
                acc[:, ns] += value

    for h in range(heads):
        hs = slice(h * HEAD_DIM, (h + 1) * HEAD_DIM)
        x = acc[:, hs] + bias[:, hs]
        turned = x * cos[...] + pltpu.roll(x, HEAD_DIM // 2, 1) * sin[...]
        plain = lax.rem(me * heads + h, GROUP) == GROUP - 1
        qkv[:, hs] = jnp.where(plain, x, turned).astype(jnp.bfloat16)

    scale = scale_ref[:, :1]
    inner = jnp.zeros((rows, 1), f32)
    for c in range(CHUNKS):
        ks = slice(c * span, (c + 1) * span)
        if c == CHUNKS - 1:
            for k in range(1, n):
                gain_copy(k).wait_recv()
            for g in range(CHUNKS):
                total = gmine[g]
                for k in range(1, n):
                    total = total + grecv[k - 1, g].astype(f32)
                for i in range(16):
                    at = g * span + i * piece
                    gg_ref[:, at:at + piece] = total[i:i + 1, :]
        ng[:, ks] = part[block(me), ks]
        for way, comes, slot in ((0, has_left, me + 1), (1, has_right, me)):
            @pl.when(comes)
            def _():
                transfer(way, run, slot, n - 1, c).wait_recv()
                ng[:, ks] += run[block(slot), ks].astype(f32)

        product = ng[:, ks] * tok[:, ks].astype(f32)
        inner = inner + jnp.sum(product * gain[:, ks], axis=1, keepdims=True)
        tg[:, ks] = scale * gain[:, ks] * ng[:, ks]

    weight = scale * scale * scale * (inner / depth)
    for c in range(CHUNKS):
        ks = slice(c * span, (c + 1) * span)
        tg[:, ks] -= tok[:, ks].astype(f32) * weight

    @pl.loop(0, n)
    def _(j):
        @pl.loop(0, CHUNKS)
        def _(c):
            for way, goes in ((0, has_right), (1, has_left)):
                @pl.when(goes)
                def _():
                    transfer(way, held, 0, j, c).wait_send()

    for k in range(1, n):
        gain_copy(k).wait_send()


def finish(qkv, tg, gg, bg, qkv_h, tg_h, gg_h, bg_h, sem):
    moves = ((qkv, qkv_h), (tg, tg_h), (gg.at[0], gg_h), (bg.at[0], bg_h))
    copies = [pltpu.make_async_copy(src, dst, sem.at[i]) for i, (src, dst) in enumerate(moves)]
    for c in copies:
        c.start()
    for c in copies:
        c.wait()


def shards(n, tokens, norm_gain, qkv_weight, qkv_bias, qkv_grad):
    rows, depth = tokens.shape
    every, width = qkv_grad.shape
    cosine, sine = rope_tables(every, rows, SEQ_LEN // n)
    bf16, f32 = jnp.bfloat16, jnp.float32
    span = depth // CHUNKS
    dma = pltpu.SemaphoreType.DMA
    hbm = pl.BlockSpec(memory_space=pl.ANY)
    vmem = pl.BlockSpec(memory_space=pltpu.VMEM)
    results = pl.pallas_call(
        functools.partial(kernel, n),
        out_shape=(
            pltpu.VMEM((every, width), bf16),
            pltpu.VMEM((rows, depth), f32),
            pltpu.VMEM((1, depth), f32),
            pltpu.VMEM((1, width), f32),
        ),
        in_specs=[hbm] * 7,
        out_specs=[vmem] * 4,
        scratch_shapes=[
            pltpu.VMEM((rows, depth), bf16),
            pltpu.VMEM((1, depth), f32),
            pltpu.VMEM((depth, width), bf16),
            pltpu.VMEM((1, width), f32),
            pltpu.VMEM((every, width), bf16),
            pltpu.VMEM((every, HEAD_DIM), f32),
            pltpu.VMEM((every, HEAD_DIM), f32),
            pltpu.VMEM((every, width), bf16),
            pltpu.VMEM((every, depth), f32),
            pltpu.VMEM((every, depth), bf16),
            pltpu.VMEM((every + rows, depth), bf16),
            pltpu.VMEM((every, width), f32),
            pltpu.VMEM((rows, depth), f32),
            pltpu.VMEM((rows, HEAD_DIM), f32),
            pltpu.VMEM((CHUNKS, 16, span // 16), f32),
            pltpu.VMEM((CHUNKS, 16, span // 16), bf16),
            pltpu.VMEM((n - 1, CHUNKS, 16, span // 16), bf16),
            dma((6,)),
            dma((depth // TILE_K,)),
            dma((2, n, CHUNKS)),
            dma((2, n, CHUNKS)),
            dma((n - 1,)),
            dma((n - 1,)),
        ],
        compiler_params=pltpu.CompilerParams(
            collective_id=0, has_side_effects=True, vmem_limit_bytes=60000000
        ),
        cost_estimate=pl.CostEstimate(
            flops=4 * every * depth * width, bytes_accessed=2 * depth * width, transcendentals=0
        ),
    )(
        tokens, norm_gain, qkv_weight, qkv_bias, qkv_grad,
        jnp.asarray(cosine), jnp.asarray(sine),
    )
    return pl.pallas_call(
        finish,
        out_shape=(
            jax.ShapeDtypeStruct((every, width), bf16),
            jax.ShapeDtypeStruct((rows, depth), f32),
            jax.ShapeDtypeStruct((depth,), f32),
            jax.ShapeDtypeStruct((width,), f32),
        ),
        in_specs=[vmem] * 4,
        out_specs=[hbm] * 4,
        scratch_shapes=[dma((4,))],
        compiler_params=pltpu.CompilerParams(vmem_limit_bytes=1 << 20),
    )(*results)


def solution(mesh):
    in_specs = (P(("dp", "mp"), None), P(), P(None, "mp"), P("mp"), P("dp", "mp"))
    out_specs = (P("dp", "mp"), P(("dp", "mp"), None), P("dp"), P(("dp", "mp")))
    body = functools.partial(shards, mesh.shape["mp"])
    return jax.shard_map(body, mesh=mesh, in_specs=in_specs, out_specs=out_specs, check_vma=False)
```
